128 devices in a mesh: fsdp: 16 (over y_hi, z, core), tensor: 8 (over y_lo, x).
Axes of the slice: x: 4, y: 4 (y_hi: 2, y_lo: 2; y = y_hi * 2 + y_lo), z: 4, core: 2. Of those that a mesh axis runs over, the one named last changes fastest.
Arguments:
- states: bfloat16 [4096, 8192], P('fsdp'), may hold values from -64 to 64
- segment_ids: int32 [16, 256], P('fsdp'), may hold values from 0 to 3, never falling along the last dimension, each value on 1 to 128 neighbouring positions
- attn_gain: float32 [8192], replicated, may hold values from 0.1 to 1.9
- query_weight: bfloat16 [8192, 4096], P('fsdp', 'tensor'), may hold values from -2 to 2
- key_weight: bfloat16 [8192, 1024], P('fsdp', 'tensor'), may hold values from -2 to 2
- value_matrix: bfloat16 [8192, 1024], P('fsdp', 'tensor'), may hold values from -0.0625 to 0.0625
- out_weight: bfloat16 [4096, 8192], P('tensor', 'fsdp'), may hold values from -0.28125 to 0.28125
- final_gain: float32 [8192], P('tensor'), may hold values from 0.1 to 1.9
- head_weight: float32 [8192], P('tensor'), may hold values from -0.0625 to 0.0625
Outputs:
- scores: float32 [4096], P(('fsdp', 'tensor'))
- resid_out: bfloat16 [4096, 8192], P('fsdp', 'tensor')
The draws below stay inside these ranges and needn't reach their ends.
Inputs may be any that keep to these rules, and one draw needn't show every extreme that they name: `segment_ids`: in each row, segment numbers never fall and each rollout spans 1 to 128 positions.
All inputs are finite; a program needn't handle non-finite values.
Results may differ from the reference program's by a relative error of at most 0.0071.
Values may be sent and summed in bfloat16 or wider, within the bound.
A program may use at most 128 MiB of HBM per device.

```python
import math
import jax
import jax.numpy as jnp
import numpy as np
from jax import lax

MODEL_WIDTH = 8192
HQ = 32
KEY_VALUE_HEADS = 8
HEAD_SIZE = 128
TOK_DEV = 256
SEG_COUNT = 4
SEG_MOST = 128
TOKENS = 4096
N_FSDP = 16


def draw_states(key, part):
    subkeys = jax.random.split(jax.random.fold_in(key, 11), 1)
    noise_part = jnp.clip(jax.random.normal(subkeys[0], (TOKENS, MODEL_WIDTH), jnp.float32), -4.0, 4.0)
    col_scale = 3.0 ** (jnp.arange(MODEL_WIDTH, dtype=jnp.float32) / MODEL_WIDTH)
    return (noise_part * col_scale[None, :]).astype(jnp.bfloat16)


def matched_weight(key, heads, salt):
    subkeys = jax.random.split(jax.random.fold_in(key, salt), 1)
    drawn_part = jnp.clip(jax.random.normal(subkeys[0], (MODEL_WIDTH, heads * HEAD_SIZE), jnp.float32), -6.0, 6.0) * MODEL_WIDTH ** (-0.5)
    return drawn_part.astype(jnp.bfloat16)


def draw_query_weight(key, part):
    return matched_weight(key, HQ, 21)


def draw_key_weight(key, part):
    return matched_weight(key, KEY_VALUE_HEADS, 31)


def shard_levels(own_key, dims, shards, smallest, high):
    def one(dim, shards_of):
        steps = jax.random.uniform(jax.random.fold_in(jax.random.fold_in(own_key, 6), dim), (shards_of,), jnp.float32, smallest / len(shards), high / len(shards))
        return jnp.repeat(jnp.exp(steps), dims[dim] // shards_of).reshape((-1,) + (1,) * (len(dims) - dim - 1))

    gain = one(*shards[0])
    for cut in shards[1:]:
        gain = gain * one(*cut)
    return gain


def split_up(count, total, most, lean):
    weights = [(1 << 20) // math.isqrt(grade ** lean) + 1 for grade in range(2, count + 1)]
    surplus, counts = total - most - (count - 1), [1] * (count - 1)
    while surplus > 0:
        free = [i for i in range(count - 1) if counts[i] < most]
        pool, left = sum([weights[i] for i in free]), surplus
        for i in free:
            addition = min(most - counts[i], max(1, left * weights[i] // pool), surplus)
            counts[i] = counts[i] + addition
            surplus = surplus - addition
    return np.array([most] + counts)


def uneven_parts(stream_key, number_of, total, limit, lean):
    if number_of == 2:
        one = jax.random.randint(stream_key, (), max(1, total - limit), min(limit, total - 1) + 1)
        return jnp.stack([one, total - one])
    tallies = jnp.asarray(split_up(number_of, total, limit, lean), jnp.int32)
    twos = (number_of - 1) // 2
    donor, taker = tallies[1:1 + 2 * twos:2], tallies[2:2 + 2 * twos:2]
    margin = jnp.minimum(donor - 1, limit - taker)
    passed = jax.random.randint(jax.random.fold_in(stream_key, 1), (twos,), 0, 1 << 20) % (margin + 1)
    tallies = tallies.at[1:1 + 2 * twos:2].set(donor - passed).at[2:2 + 2 * twos:2].set(taker + passed)
    return tallies[jax.random.permutation(jax.random.fold_in(stream_key, 2), number_of)]


def bell_draw(key, shape, scale, limit, shards=(), kind=jnp.bfloat16):
    factor_of = shard_levels(key, shape, shards, -0.22, 0.18) if shards else 1.0
    entries = jax.random.normal(key, shape, jnp.float32) * scale * factor_of
    return jnp.minimum(jnp.maximum(entries, -limit), limit).astype(kind)


def setup_inputs(seed: int = 0) -> dict:
    splits = jax.random.split(jax.random.key(seed), 10)
    states = draw_states(jax.random.fold_in(splits[9], 71), 0)
    segment_ids = jax.vmap(lambda own: jnp.searchsorted(jnp.cumsum(uneven_parts(own, SEG_COUNT, TOK_DEV, SEG_MOST, 1)), jnp.arange(TOK_DEV), side="right"))(jax.random.split(splits[1], N_FSDP)).reshape((N_FSDP, TOK_DEV)).astype(jnp.int32)
    attn_gain = jnp.clip(1.0 + 0.18 * jax.random.normal(splits[2], (MODEL_WIDTH,), jnp.float32), 0.1, 1.9)
    query_weight = draw_query_weight(jax.random.fold_in(splits[9], 71), 0)
    key_weight = draw_key_weight(jax.random.fold_in(splits[9], 71), 0)
    value_matrix = bell_draw(splits[5], (MODEL_WIDTH, KEY_VALUE_HEADS * HEAD_SIZE), MODEL_WIDTH ** -0.5, 0.0625, ((0, 16), (1, 8)))
    out_weight = bell_draw(splits[6], (HQ * HEAD_SIZE, MODEL_WIDTH), (3.0 / (HQ * HEAD_SIZE) ** 0.5), 0.28125, ((0, 8), (1, 16)))
    final_gain = jnp.clip(1.0 + 0.18 * jax.random.normal(splits[7], (MODEL_WIDTH,), jnp.float32), 0.1, 1.9)
    head_weight = bell_draw(splits[8], (MODEL_WIDTH,), MODEL_WIDTH ** -0.5, 0.0625, ((0, 8),), jnp.float32)
    return dict(states=states, segment_ids=segment_ids, attn_gain=attn_gain, query_weight=query_weight, key_weight=key_weight, value_matrix=value_matrix, out_weight=out_weight, final_gain=final_gain, head_weight=head_weight)


EPS = 1e-05
THETA = 500000.0
NEG_FILL = -1e+30

def rope_tables(seg_row):
    count = seg_row.shape[0]
    places = jnp.arange(count, dtype=jnp.int32)
    boundary = jnp.concatenate([jnp.ones((1,), dtype=bool), seg_row[1:] != seg_row[:-1]])
    begins = lax.cummax(jnp.where(boundary, places, jnp.zeros_like(places)), axis=0)
    positions = (places - begins).astype(jnp.float32)
    half_width = HEAD_SIZE // 2
    frequency = THETA ** (-(2.0 * jnp.arange(half_width, dtype=jnp.float32)) / HEAD_SIZE)
    angles = positions[:, None] * frequency[None, :]
    return (jnp.cos(angles), jnp.sin(angles))

def rotated(block, cosine, sine_part):
    half_width = block.shape[-1] // 2
    first_half = block[..., :half_width]
    second_half = block[..., half_width:]
    cos_rows = cosine[:, None, :]
    sin_rows = sine_part[:, None, :]
    return jnp.concatenate([first_half * cos_rows - second_half * sin_rows, second_half * cos_rows + first_half * sin_rows], axis=-1)

def attend(queries, key_rows, values, seg_row):
    t_rows = queries.shape[0]
    heads_here = queries.shape[1] // HEAD_SIZE
    groups_here = key_rows.shape[1] // HEAD_SIZE
    ratio = heads_here // groups_here
    cosine, sine_part = rope_tables(seg_row)
    query_rot = rotated(queries.reshape(t_rows, heads_here, HEAD_SIZE), cosine, sine_part).astype(jnp.bfloat16)
    key_rot = rotated(key_rows.reshape(t_rows, groups_here, HEAD_SIZE), cosine, sine_part).astype(jnp.bfloat16)
    value_rows = values.astype(jnp.bfloat16).reshape(t_rows, groups_here, HEAD_SIZE)
    grouped = query_rot.reshape(t_rows, groups_here, ratio, HEAD_SIZE)
    logits = jnp.einsum('tkgd,skd->kgts', grouped.astype(jnp.float32), key_rot.astype(jnp.float32)) * HEAD_SIZE ** (-0.5)
    places = jnp.arange(t_rows, dtype=jnp.int32)
    allowed = (seg_row[:, None] == seg_row[None, :]) & (places[None, :] <= places[:, None])
    logits = jnp.where(allowed[None, None], logits, NEG_FILL)
    row_peak = lax.optimization_barrier(jnp.max(logits, axis=-1, keepdims=True))
    raised = jnp.exp(logits - row_peak)
    probabilities = (raised / lax.optimization_barrier(jnp.sum(raised, axis=-1, keepdims=True))).astype(jnp.bfloat16)
    mixed = jnp.einsum('kgts,skd->tkgd', probabilities.astype(jnp.float32), value_rows.astype(jnp.float32))
    return mixed.astype(jnp.bfloat16).reshape(t_rows, heads_here * HEAD_SIZE)

def reference(states, segment_ids, attn_gain, query_weight, key_weight, value_matrix, out_weight, final_gain, head_weight):
    widened = states.astype(jnp.float32)
    normed = (widened * lax.rsqrt(lax.optimization_barrier(jnp.sum(widened * widened, axis=1, keepdims=True)) / MODEL_WIDTH + EPS) * attn_gain[None, :]).astype(jnp.bfloat16)
    normed_blocks = normed.reshape(N_FSDP, TOK_DEV, MODEL_WIDTH)

    def single_block(operands):
        block_rows, seg_row = operands
        queries = jnp.dot(block_rows, query_weight, preferred_element_type=jnp.float32)
        key_rows = jnp.dot(block_rows, key_weight, preferred_element_type=jnp.float32)
        values = jnp.dot(block_rows, value_matrix, preferred_element_type=jnp.float32)
        return attend(queries, key_rows, values, seg_row)
    mixed = lax.map(single_block, (normed_blocks, segment_ids)).reshape(TOKENS, HQ * HEAD_SIZE)
    branch = jnp.dot(mixed, out_weight, preferred_element_type=jnp.float32)
    resid_out = (widened + branch).astype(jnp.bfloat16)
    stream = resid_out.astype(jnp.float32)
    squares = lax.optimization_barrier(jnp.sum(stream * stream, axis=1))
    products = lax.optimization_barrier(jnp.sum(stream * (final_gain * head_weight)[None, :], axis=1))
    scores = products * lax.rsqrt(squares / MODEL_WIDTH + EPS)
    return (scores, resid_out)
```

```python
import functools

import jax
import jax.numpy as jnp
import numpy as np
from jax import lax
from jax.experimental import pallas as pl
from jax.experimental.pallas import tpu as pltpu
from jax.sharding import PartitionSpec as P

WIDTH = 8192
HEAD = 128
HEADS_HERE = 4
TOK = 256
EPS = 1e-05
THETA = 500000.0
NEG_FILL = -1e30
MESH = pl.DeviceIdType.MESH
F32 = jnp.float32
BF16 = jnp.bfloat16

ORIGINS = ((0, 0), (0, -1), (0, 1), (1, 0), (0, 2), (1, -1), (1, 1), (1, 2))
ROWS = 512
SPLIT_QKV = 288
SPLIT_OUT = 384
KINDS = ("x", "x", "x", "x", "x", "x", "x", "x")
N_SEM = 160


def kernel(
    states_hbm, seg_ref, gain_ref, q_hbm, k_hbm, v_hbm, o_hbm, fg_ref, hw_ref, freq_ref,
    scores_ref, resid_ref,
    st, normed, wqkv, wout, acc, mixed, part, xin, yin, ssum, res, fgs, hws,
    lsem, ssem, rsem,
):
    f = lax.axis_index("fsdp")
    t = lax.axis_index("tensor")
    core = lax.rem(f, 2)
    zz = lax.rem(f // 2, 4)
    yh = f // 8
    yl = t // 4
    xx = lax.rem(t, 4)

    def fdev(dy, dz, other_core=False):
        y2 = 1 - yh if dy else yh
        z2 = lax.rem(zz + dz + 4, 4)
        c2 = 1 - core if other_core else core
        return (y2 * 4 + z2) * 2 + c2

    def pair_of(origin):
        y2 = 1 - yh if origin[0] else yh
        return y2 * 4 + lax.rem(zz + origin[1] + 4, 4)

    zp, zm, ypart, sib = (fdev(0, 1), t), (fdev(0, -1), t), (fdev(1, 0), t), (fdev(0, 0, True), t)
    xpeer = [(f, yl * 4 + lax.rem(xx + d, 4)) for d in (1, 2, 3)]
    tpeer = [(f, lax.rem(t + d, 8)) for d in range(1, 8)]

    barrier = pltpu.get_barrier_semaphore()
    peers = [zp, zm, ypart, sib] + tpeer
    for d in peers:
        pl.semaphore_signal(barrier, inc=1, device_id=d, device_id_type=MESH)

    own_q = pltpu.make_async_copy(q_hbm, wqkv.at[f // 2, pl.ds(core * ROWS, ROWS), pl.ds(0, 512)], lsem.at[0])
    own_k = pltpu.make_async_copy(k_hbm, wqkv.at[f // 2, pl.ds(core * ROWS, ROWS), pl.ds(512, 128)], lsem.at[1])
    own_v = pltpu.make_async_copy(v_hbm, wqkv.at[f // 2, pl.ds(core * ROWS, ROWS), pl.ds(640, 128)], lsem.at[2])
    own_s = pltpu.make_async_copy(states_hbm, st, lsem.at[3])
    own_o = pltpu.make_async_copy(o_hbm, wout.at[f // 2, core], lsem.at[4])
    for cp in (own_q, own_k, own_v, own_s, own_o):
        cp.start()

    ids = {}

    def sem_id(name):
        return ids.setdefault(name, len(ids))

    sent = []

    def send(src, dst, device, name):
        i = sem_id(name)
        cp = pltpu.make_async_remote_copy(
            src_ref=src, dst_ref=dst, send_sem=ssem.at[i], recv_sem=rsem.at[i],
            device_id=device, device_id_type=MESH,
        )
        cp.start()
        sent.append(cp)

    def arrived(dst, name):
        i = sem_id(name)
        pltpu.make_async_remote_copy(
            src_ref=dst, dst_ref=dst, send_sem=ssem.at[i], recv_sem=rsem.at[i],
            device_id=zp, device_id_type=MESH,
        ).wait_recv()

    class Gather:
        def __init__(self, tag, split):
            self.tag = tag
            h = split // 2
            g = (ROWS - split) // 2
            self.span = {
                "1": (0, split), "1A": (0, h), "1B": (h, split - h),
                "2": (split, ROWS - split), "2A": (split, g), "2B": (split + g, ROWS - split - g),
                "all": (0, ROWS),
            }

        def at(self, origin, piece, mine=True):
            lo, n = self.span[piece]
            c = core if mine else 1 - core
            if self.tag == "q":
                return wqkv.at[pair_of(origin), pl.ds(pl.multiple_of(c * ROWS + lo, 16), n), :]
            return wout.at[pair_of(origin), c, pl.ds(lo, n), :]

        def name(self, origin, piece):
            return (self.tag, origin, piece)

        def send(self, origin, piece, device, seen_as):
            ref = self.at(origin, piece)
            send(ref, ref, device, self.name(seen_as, piece))

        def wait(self, origin, piece):
            arrived(self.at(origin, piece), self.name(origin, piece))

        def cross(self, origin):
            ref = self.at(origin, "all")
            send(ref, ref, sib, (self.tag, origin, "sib"))

        def wait_cross(self, origin):
            arrived(self.at(origin, "all", mine=False), (self.tag, origin, "sib"))

        def s0(self):
            o = (0, 0)
            self.send(o, "1", ypart, (1, 0))
            self.send(o, "1", zp, (0, -1))
            self.send(o, "1", zm, (0, 1))
            self.send(o, "2", zp, (0, -1))
            self.send(o, "2", zm, (0, 1))
            self.send(o, "2", ypart, (1, 0))
            self.cross(o)

        def s1(self):
            self.wait((1, 0), "1")
            self.send((1, 0), "1", zp, (1, -1))
            self.send((1, 0), "1", zm, (1, 1))

        def s2(self):
            self.wait((0, -1), "2")
            self.send((0, -1), "2A", zp, (0, 2))
            self.send((0, -1), "2", ypart, (1, -1))
            self.wait((0, 1), "2")
            self.send((0, 1), "2B", zm, (0, 2))
            self.send((0, 1), "2", ypart, (1, 1))

        def s3(self):
            self.wait((0, -1), "1")
            self.send((0, -1), "1A", zp, (0, 2))
            self.wait((0, 1), "1")
            self.send((0, 1), "1B", zm, (0, 2))
            self.cross((0, -1))
            self.cross((0, 1))
            self.wait((1, 0), "2")
            self.cross((1, 0))

        def s4(self):
            self.wait((1, -1), "1")
            self.send((1, -1), "1A", zp, (1, 2))
            self.wait((1, 1), "1")
            self.send((1, 1), "1B", zm, (1, 2))

        def s5(self):
            self.wait((0, 2), "2A")
            self.send((0, 2), "2A", ypart, (1, 2))
            self.wait((0, 2), "2B")
            self.send((0, 2), "2B", ypart, (1, 2))

        def s6(self):
            self.wait((0, 2), "1A")
            self.wait((0, 2), "1B")
            self.cross((0, 2))

        def s7(self):
            self.wait((1, -1), "2")
            self.cross((1, -1))
            self.wait((1, 1), "2")
            self.cross((1, 1))

        def s8(self):
            for piece in ("1A", "1B", "2A", "2B"):
                self.wait((1, 2), piece)
            self.cross((1, 2))

    gq = Gather("q", SPLIT_QKV)
    go = Gather("o", SPLIT_OUT)

    own_q.wait()
    own_k.wait()
    own_v.wait()
    pl.semaphore_wait(barrier, len(peers))
    gq.s0()
    for n, d in enumerate(tpeer):
        send(fg_ref, fgs.at[t], d, ("fg", n))
        send(hw_ref, hws.at[t], d, ("hw", n))
    fgs[t] = fg_ref[...]
    hws[t] = hw_ref[...]

    own_s.wait()
    acc[...] = jnp.zeros_like(acc)

    @pl.loop(0, TOK // 32)
    def _(rb):
        rows = pl.ds(pl.multiple_of(rb * 32, 32), 32)
        total = jnp.zeros((32, 128), F32)
        for cb in range(WIDTH // 512):
            v = st[rows, cb * 512:(cb + 1) * 512].astype(F32)
            v = v * v
            total += v[:, :128] + v[:, 128:256] + v[:, 256:384] + v[:, 384:]
        scale = lax.rsqrt(jnp.sum(total, axis=1, keepdims=True) / WIDTH + EPS)
        for cb in range(WIDTH // 512):
            v = st[rows, cb * 512:(cb + 1) * 512].astype(F32)
            g = gain_ref[:, cb * 512:(cb + 1) * 512]
            normed[rows, cb * 512:(cb + 1) * 512] = (v * scale * g).astype(BF16)

    def project(origin):
        gq.wait_cross(origin)
        p = pair_of(origin)
        cols = pl.ds(pl.multiple_of(p * 1024, 1024), 1024)
        acc[...] += jnp.dot(normed[:, cols], wqkv[p], preferred_element_type=F32)

    project((0, 0))

    seg_row = seg_ref[...].astype(F32)
    row_i = lax.broadcasted_iota(jnp.int32, (TOK, TOK), 0)
    col_i = lax.broadcasted_iota(jnp.int32, (TOK, TOK), 1)
    seg_all = jnp.broadcast_to(seg_row, (TOK, TOK))
    seg_col = jnp.sum(jnp.where(row_i == col_i, seg_all, 0.0), axis=1, keepdims=True)
    same = seg_all == seg_col
    first = jnp.min(jnp.where(same, col_i.astype(F32), 1e9), axis=1, keepdims=True)
    position = lax.broadcasted_iota(jnp.int32, (TOK, 1), 0).astype(F32) - first
    allowed = same & (col_i <= row_i)
    angle = position * freq_ref[...]
    cos2 = jnp.cos(angle)
    sin2 = jnp.sin(angle)
    lane = lax.broadcasted_iota(jnp.int32, (TOK, HEAD), 1)
    sin2 = jnp.where(lane < HEAD // 2, -sin2, sin2)

    gq.s1()
    gq.s2()
    gq.s3()
    project((0, -1))
    project((0, 1))
    project((1, 0))
    gq.s4()
    gq.s5()
    own_o.wait()
    go.s0()
    gq.s6()
    gq.s7()
    project((0, 2))
    project((1, -1))
    project((1, 1))
    gq.s8()
    project((1, 2))

    def rotate(block):
        return (block * cos2 + pltpu.roll(block, HEAD // 2, 1) * sin2).astype(BF16)

    key_rot = rotate(acc[:, 512:640])
    value_rows = acc[:, 640:768].astype(BF16)
    for h in range(HEADS_HERE):
        query_rot = rotate(acc[:, h * HEAD:(h + 1) * HEAD])
        logits = lax.dot_general(
            query_rot, key_rot, (((1,), (1,)), ((), ())), preferred_element_type=F32
        ) * HEAD ** (-0.5)
        logits = jnp.where(allowed, logits, NEG_FILL)
        raised = jnp.exp(logits - jnp.max(logits, axis=1, keepdims=True))
        probs = (raised / jnp.sum(raised, axis=1, keepdims=True)).astype(BF16)
        out = jnp.dot(probs, value_rows, preferred_element_type=F32)
        mixed[:, h * HEAD:(h + 1) * HEAD] = out.astype(BF16)

    sums = [jnp.zeros((32, 128), F32), jnp.zeros((32, 128), F32)]

    def expand(n):
        origin = ORIGINS[n]
        go.wait_cross(origin)
        p = pair_of(origin)
        for j in range(2):
            block = jnp.dot(mixed[...], wout[p, j], preferred_element_type=F32)
            part[n, :, :, :, j * 512:(j + 1) * 512] = block.astype(BF16).reshape(2, 4, 32, 512)
        if KINDS[n] == "x":
            for d in range(3):
                send(part.at[n, :, xpeer[d][1] - yl * 4], xin.at[n, d], xpeer[d], ("rs1", n, d))
        else:
            send(part.at[n, 1 - yl], yin.at[n], (f, (1 - yl) * 4 + xx), ("rs1", n))

    def middle(n):
        if KINDS[n] == "x":
            total = part[n, :, xx].astype(F32)
            for d in range(3):
                arrived(xin.at[n, d], ("rs1", n, d))
                total += xin[n, d].astype(F32)
            ssum[n, 0:2] = total.astype(BF16)
            send(ssum.at[n, 1 - yl], yin.at[n, 0], (f, (1 - yl) * 4 + xx), ("rs2", n))
        else:
            arrived(yin.at[n], ("rs1", n))
            ssum[n] = (part[n, yl].astype(F32) + yin[n].astype(F32)).astype(BF16)
            for d in range(3):
                send(ssum.at[n, xpeer[d][1] - yl * 4], xin.at[n, d, 0], xpeer[d], ("rs2", n, d))

    res_sends = []

    def finish(n):
        p = pair_of(ORIGINS[n])
        if KINDS[n] == "x":
            arrived(yin.at[n, 0], ("rs2", n))
            total = ssum[n, yl].astype(F32) + yin[n, 0].astype(F32)
        else:
            total = ssum[n, xx].astype(F32)
            for d in range(3):
                arrived(xin.at[n, d, 0], ("rs2", n, d))
                total += xin[n, d, 0].astype(F32)
        cols = pl.ds(pl.multiple_of(p * 1024, 1024), 1024)
        mine = st[pl.ds(pl.multiple_of(t * 32, 32), 32), cols].astype(F32)
        out = (mine + total).astype(BF16)
        res[n] = out
        stream = out.astype(F32)
        gh = fgs[p] * hws[p]
        sq = stream * stream
        pr = stream * gh
        for b in range(8):
            sums[0] += sq[:, b * 128:(b + 1) * 128]
            sums[1] += pr[:, b * 128:(b + 1) * 128]
        i = sem_id(("res", n))
        cp = pltpu.make_async_remote_copy(
            src_ref=res.at[n], dst_ref=resid_ref.at[pl.ds(pl.multiple_of(t * 32, 32), 32), :],
            send_sem=ssem.at[i], recv_sem=rsem.at[N_SEM + t],
            device_id=(f, p), device_id_type=MESH,
        )
        res_sends.append((p, cp))

        @pl.when(p != t)
        def _():
            cp.start()

        @pl.when(p == t)
        def _():
            resid_ref[pl.ds(pl.multiple_of(t * 32, 32), 32), :] = out

    for n, d in enumerate(tpeer):
        src = lax.rem(t + 8 - (n + 1), 8)
        arrived(fgs.at[src], ("fg", n))
        arrived(hws.at[src], ("hw", n))

    expand(0)
    go.s1()
    go.s2()
    go.s3()
    expand(1)
    expand(2)
    go.s4()
    go.s5()
    expand(3)
    middle(0)
    go.s6()
    expand(4)
    middle(1)
    go.s7()
    expand(5)
    expand(6)
    middle(2)
    go.s8()
    expand(7)
    finish(0)
    middle(3)
    finish(1)
    middle(4)
    finish(2)
    middle(5)
    finish(3)
    middle(6)
    finish(4)
    middle(7)
    finish(5)
    finish(6)
    finish(7)

    squares = jnp.sum(sums[0], axis=1, keepdims=True)
    products = jnp.sum(sums[1], axis=1, keepdims=True)
    scores_ref[...] = products * lax.rsqrt(squares / WIDTH + EPS)

    for d in range(1, 8):
        src = lax.rem(t + d, 8)
        rows = resid_ref.at[pl.ds(pl.multiple_of(src * 32, 32), 32), :]
        pltpu.make_async_remote_copy(
            src_ref=rows, dst_ref=rows, send_sem=ssem.at[0], recv_sem=rsem.at[N_SEM + src],
            device_id=zp, device_id_type=MESH,
        ).wait_recv()
    for cp in sent:
        cp.wait_send()
    for p, cp in res_sends:
        @pl.when(p != t)
        def _():
            cp.wait_send()
    assert len(ids) <= N_SEM, len(ids)


def body(states, segment_ids, attn_gain, query_weight, key_weight, value_matrix, out_weight,
         final_gain, head_weight):
    half = HEAD // 2
    freq = THETA ** (-(2.0 * jnp.arange(half, dtype=F32)) / HEAD)
    freq = jnp.concatenate([freq, freq]).reshape(1, HEAD)
    hbm = pl.BlockSpec(memory_space=pl.ANY)
    vmem = pl.BlockSpec(memory_space=pltpu.VMEM)
    n = len(ORIGINS)
    scores, resid = pl.pallas_call(
        kernel,
        out_shape=(
            jax.ShapeDtypeStruct((32, 1), F32),
            jax.ShapeDtypeStruct((TOK, 1024), BF16),
        ),
        in_specs=[hbm, vmem, vmem, hbm, hbm, hbm, hbm, vmem, vmem, vmem],
        out_specs=(vmem, vmem),
        scratch_shapes=[
            pltpu.VMEM((TOK, WIDTH), BF16),
            pltpu.VMEM((TOK, WIDTH), BF16),
            pltpu.VMEM((8, 1024, 768), BF16),
            pltpu.VMEM((8, 2, 512, 512), BF16),
            pltpu.VMEM((TOK, 768), F32),
            pltpu.VMEM((TOK, 512), BF16),
            pltpu.VMEM((n, 2, 4, 32, 1024), BF16),
            pltpu.VMEM((n, 3, 2, 32, 1024), BF16),
            pltpu.VMEM((n, 4, 32, 1024), BF16),
            pltpu.VMEM((n, 4, 32, 1024), BF16),
            pltpu.VMEM((n, 32, 1024), BF16),
            pltpu.VMEM((8, 1, 1024), F32),
            pltpu.VMEM((8, 1, 1024), F32),
            pltpu.SemaphoreType.DMA((5,)),
            pltpu.SemaphoreType.DMA((N_SEM,)),
            pltpu.SemaphoreType.DMA((N_SEM + 8,)),
        ],
        compiler_params=pltpu.CompilerParams(
            collective_id=0, has_side_effects=True, vmem_limit_bytes=62 * 1024 * 1024
        ),
        name="critic",
    )(
        states, segment_ids, attn_gain.reshape(1, WIDTH), query_weight, key_weight, value_matrix,
        out_weight, final_gain.reshape(1, 1024), head_weight.reshape(1, 1024), freq,
    )
    return scores.reshape(32), resid


def solution(mesh):
    placed = (
        P("fsdp", None), P("fsdp", None), P(), P("fsdp", "tensor"), P("fsdp", "tensor"),
        P("fsdp", "tensor"), P("tensor", "fsdp"), P("tensor"), P("tensor"),
    )
    return jax.shard_map(
        body, mesh=mesh, in_specs=placed,
        out_specs=(P(("fsdp", "tensor")), P("fsdp", "tensor")), check_vma=False,
    )
```
